32 devices in a mesh: dp: 8 (over y, x, core), tp: 4 (over z).
Axes of the slice: x: 2, y: 2, z: 4, core: 2. Of those that a mesh axis runs over, the one named last changes fastest.
Arguments:
- embeddings: bfloat16 [768, 192, 256], P(('dp', 'tp')), may hold values from -6 to 6
- projection: bfloat16 [256, 16], replicated, may hold values from -0.375 to 0.375
- compress: bfloat16 [256, 4], replicated, may hold values from -0.375 to 0.375
- w_up: bfloat16 [4096, 4096], P(None, 'tp'), may hold values from -0.09375 to 0.09375
- w_down: bfloat16 [4096, 768], P('tp'), may hold values from -0.125 to 0.125
- output_norm_gain: float32 [1536], P('tp'), may hold values from 0.25 to 1.75
- out_grad: bfloat16 [768, 1536], P('dp', 'tp'), may hold values from -6 to 6
Outputs:
- block_result: bfloat16 [768, 1536], P('dp', 'tp')
- grad_down: float32 [4096, 768], P(('tp', 'dp'))
The draws below stay inside these ranges and needn't reach their ends.
All inputs are finite; a program needn't handle non-finite values.
Results may differ from the reference program's by a relative error of at most 0.017.
Values may be sent and summed in bfloat16 or wider, within the bound.
A program may use at most 64 MiB of HBM per device.

```python
import jax
import jax.numpy as jnp
from jax import lax

FIELDS = 256
EDIM = 192
RANK = 16
HIDDEN_SIZE = 4096
NL = 4
FEAT = 4096
FMW = 768
DOUT = 1536
BATCH = 768
N_TP = 4


def strengthened(entries, stream_key, source, target, shards_of, factor):
    def block_of(axis_at):
        return (jnp.arange(entries.shape[axis_at]) // (entries.shape[axis_at] // shards_of)).reshape((-1,) + (1,) * (entries.ndim - 1 - axis_at))

    near = jax.random.permutation(stream_key, shards_of)[block_of(target)]
    far = (block_of(target) + shards_of // 2) % shards_of
    return jnp.where((block_of(source) == near) | (block_of(source) == far), factor * entries, entries)


def shard_levels(rng, shape, shards, smallest, largest):
    loudness, own = 1.0, jax.random.fold_in(rng, 6)
    for axis_at, blocks in shards:
        heights = jnp.exp(jax.random.uniform(jax.random.fold_in(own, axis_at), (blocks,), jnp.float32, smallest / len(shards), largest / len(shards)))
        loudness = loudness * jnp.repeat(heights, shape[axis_at] // blocks).reshape([-1 if axis == axis_at else 1 for axis in range(len(shape))])
    return loudness


def gaussian(own_key, shape, deviation, most, split=(), dtype=jnp.bfloat16):
    array = jax.random.normal(own_key, shape, jnp.float32) * deviation
    if len(split) > 0:
        array = shard_levels(own_key, shape, split, -0.22, 0.18) * array
    return jnp.clip(array, min=-most, max=most).astype(dtype)


def bell_draw_with(rng, shape, scale, most, shards, heavy, dtype=jnp.bfloat16):
    values = scale * jax.random.normal(rng, shape, jnp.float32)
    if shards:
        values = values * shard_levels(rng, shape, shards, -0.22, 0.18)
    return jnp.clip(strengthened(values, jax.random.fold_in(rng, 3), *heavy), -most, most).astype(dtype)


def setup_inputs(seed: int = 0) -> dict:
    splits = jax.random.split(jax.random.key(seed), 8)
    embeddings = gaussian(splits[0], (BATCH, EDIM, FIELDS), 1.0, 6.0, ((0, 32),))
    projection = gaussian(splits[1], (FIELDS, RANK), FIELDS ** -0.5, 0.375)
    compress = gaussian(splits[2], (FIELDS, NL), FIELDS ** -0.5, 0.375)
    w_up = gaussian(splits[3], (FEAT, HIDDEN_SIZE), FEAT ** -0.5, 0.09375, ((1, 4),))
    w_down = bell_draw_with(splits[4], (HIDDEN_SIZE, FMW), HIDDEN_SIZE ** -0.5, 0.125, ((0, 4),), (0, 1, 4, 2.0))
    output_norm_gain = jnp.clip(1.0 + 0.15 * jax.random.normal(splits[5], (DOUT,), jnp.float32), 0.25, 1.75)
    out_grad = gaussian(splits[6], (BATCH, DOUT), 1.0, 6.0, ((0, 8), (1, 4)))
    return dict(embeddings=embeddings, projection=projection, compress=compress, w_up=w_up, w_down=w_down, output_norm_gain=output_norm_gain, out_grad=out_grad)


def interact(block, projection, compress):
    x32 = block.astype(jnp.float32)
    pairs = jnp.einsum('sef,fk->sek', x32, projection.astype(jnp.float32)).astype(jnp.bfloat16)
    inter = jnp.einsum('sek,sef->skf', pairs.astype(jnp.float32), x32)
    inter = inter.reshape(block.shape[0], -1)
    center = inter - lax.optimization_barrier(jnp.mean(inter, axis=1, keepdims=True))
    spread = lax.optimization_barrier(jnp.mean(center * center, axis=1, keepdims=True))
    normed = (center / jnp.sqrt(spread + 1e-05)).astype(jnp.bfloat16)
    lcb = jnp.einsum('sef,fj->sje', x32, compress.astype(jnp.float32)).reshape(block.shape[0], -1)
    return (normed, lcb)

def reference(embeddings, projection, compress, w_up, w_down, output_norm_gain, out_grad):
    blocks = embeddings.reshape(-1, 256, embeddings.shape[1], embeddings.shape[2]) if embeddings.shape[0] % 256 == 0 else embeddings.reshape(1, embeddings.shape[0], embeddings.shape[1], embeddings.shape[2])
    normed, lcb = lax.map(lambda b: interact(b, projection, compress), blocks)
    rows = embeddings.shape[0]
    normed = normed.reshape(rows, -1)
    lcb = lcb.reshape(rows, -1)
    hidden = jax.nn.gelu(jnp.dot(normed, w_up, preferred_element_type=jnp.float32), approximate=True).astype(jnp.bfloat16)
    mlp = jnp.dot(hidden, w_down, preferred_element_type=jnp.float32)
    group_mlp = mlp.shape[1] // N_TP
    mixed_rows = jnp.concatenate([mlp.reshape(rows, N_TP, -1), lcb.reshape(rows, N_TP, -1)], axis=2).reshape(rows, -1)
    row_average = lax.optimization_barrier(jnp.mean(mixed_rows, axis=1, keepdims=True))
    var = lax.optimization_barrier(jnp.mean((mixed_rows - row_average) ** 2, axis=1, keepdims=True))
    inverse_deviation = 1.0 / jnp.sqrt(var + 1e-05)
    centered_rows = (mixed_rows - row_average) * inverse_deviation
    block_result = (centered_rows * output_norm_gain).astype(jnp.bfloat16)
    scaled_rows = out_grad.astype(jnp.float32) * output_norm_gain
    first_moment = lax.optimization_barrier(jnp.mean(scaled_rows, axis=1, keepdims=True))
    second_moment = lax.optimization_barrier(jnp.mean(scaled_rows * centered_rows, axis=1, keepdims=True))
    mixed_gradient = ((scaled_rows - first_moment - centered_rows * second_moment) * inverse_deviation).astype(jnp.bfloat16)
    mlp_grad = mixed_gradient.reshape(rows, N_TP, -1)[:, :, :group_mlp].reshape(rows, -1)
    grad_down = jnp.dot(hidden.T, mlp_grad, preferred_element_type=jnp.float32)
    return (block_result, grad_down)
```

```python
import functools

import jax
import jax.numpy as jnp
from jax import lax
from jax.experimental import pallas as pl
from jax.experimental.pallas import tpu as pltpu
from jax.sharding import PartitionSpec as P

CHUNKS = 4
EPS = 1e-05


def fused_kernel(
    dp, tp, samples, rows, group,
    norm_ref, lcb_ref, up_hbm, down_hbm, gain_ref, cot_ref,
    res_ref, grad_ref,
    up, down, gathered, lcb_in, acc, hid, hid_in, part, part_in, stat, stat_in, dmix, half_out, half_in,
    load_sem, ag_send, ag_recv, lcb_send, lcb_recv, hid_send, hid_recv, part_send, part_recv,
    stat_send, stat_recv, col_send, col_recv, x_send, x_recv, y_send, y_recv, d_send, d_recv, c_send, c_recv,
):
    me = lax.axis_index("tp")
    ring = lax.axis_index("dp")
    core = lax.rem(ring, 2)
    east = lax.rem(ring // 2, 2)
    north = ring // 4
    x_peer = ring + 2 - 4 * east
    y_peer = ring + 4 - 8 * north
    d_peer = x_peer + 4 - 8 * north
    c_peer = ring + 1 - 2 * core
    chip = ring // 2
    half = rows // 2
    tall = 2 * samples
    feats = norm_ref.shape[2]
    width = 2 * group

    loads = []
    for c in range(CHUNKS):
        piece = pl.ds(c * 2 * feats, 2 * feats)
        loads.append(pltpu.make_async_copy(up_hbm.at[piece], up.at[piece], load_sem.at[c]))
    loads.append(pltpu.make_async_copy(down_hbm, down, load_sem.at[CHUNKS]))
    for load in loads:
        load.start()

    peers = [{"tp": lax.rem(me + k, tp)} for k in range(1, tp)]
    others = [{"dp": x_peer}, {"dp": y_peer}, {"dp": d_peer}, {"dp": c_peer}]
    barrier = pltpu.get_barrier_semaphore()
    for peer in peers + others:
        pl.semaphore_signal(barrier, inc=1, device_id=peer, device_id_type=pl.DeviceIdType.MESH)
    pl.semaphore_wait(barrier, tp + 3)

    def remote(src, dst, send, recv, peer):
        return pltpu.make_async_remote_copy(
            src_ref=src, dst_ref=dst, send_sem=send, recv_sem=recv,
            device_id=peer, device_id_type=pl.DeviceIdType.MESH,
        )

    def block_rows(owner):
        return pl.ds(pl.multiple_of(owner * tall, tall), tall)

    def hop(way, d, c):
        step = 1 if way == 0 else -1
        owner = me - step * d
        dst = gathered.at[c, block_rows(owner)]
        src = norm_ref.at[c] if d == 0 else dst
        return remote(src, dst, ag_send.at[way, d, c], ag_recv.at[way, d + 1, c],
                      {"tp": lax.rem(me + step + tp, tp)})

    def arrival(way, d, c):
        step = 1 if way == 0 else -1
        owner = me - step * d
        dst = gathered.at[c, block_rows(owner)]
        return remote(dst, dst, ag_send.at[way, d, c], ag_recv.at[way, d, c],
                      {"tp": lax.rem(me + step + tp, tp)})

    def sends(way, d):
        return (me >= d) & (me < tp - 1) if way == 0 else (me < tp - d) & (me > 0)

    def gets(way, d):
        return me >= d if way == 0 else me < tp - d

    for way in range(2):
        @pl.when(sends(way, 0))
        def _():
            for c in range(CHUNKS):
                hop(way, 0, c).start()
    for c in range(CHUNKS):
        gathered[c, block_rows(me)] = norm_ref[c]
    lcb_in[me] = lcb_ref[me]

    def lcb_copy(k):
        return remote(lcb_ref.at[lax.rem(me + k, tp)], lcb_in.at[me], lcb_send.at[k], lcb_recv.at[k], peers[k - 1])

    def lcb_arrival(k):
        src = lax.rem(me - k + tp, tp)
        return remote(lcb_in.at[src], lcb_in.at[src], lcb_send.at[k], lcb_recv.at[k], peers[k - 1])

    for d in range(1, tp):
        if d == tp - 1:
            for k in range(1, tp):
                lcb_copy(k).start()
        for c in range(CHUNKS):
            for way in range(2):
                @pl.when(gets(way, d))
                def _():
                    arrival(way, d, c).wait_recv()
                if d < tp - 1:
                    @pl.when(sends(way, d))
                    def _():
                        hop(way, d, c).start()
            if d == tp - 1:
                loads[c].wait()
                for side in range(2):
                    term = jnp.dot(gathered[c], up[pl.ds((2 * c + side) * feats, feats), :],
                                   preferred_element_type=jnp.float32)
                    if c == 0:
                        acc[side] = term
                    else:
                        acc[side] += term

    for t in range(tp):
        total = acc[0, t * tall:t * tall + samples] + acc[1, t * tall + samples:(t + 1) * tall]
        acc[0, t * samples:(t + 1) * samples] = total
    chips = dp // 2
    span = hid.shape[2]
    for q in range(chips):
        hid[q] = jax.nn.gelu(acc[0, :rows, q * span:(q + 1) * span], approximate=True).astype(jnp.bfloat16)

    def hid_copy(slot, peer):
        return remote(hid.at[peer // 2], hid_in.at[slot], hid_send.at[slot], hid_recv.at[slot], {"dp": peer})

    hid_copies = [hid_copy(1, x_peer), hid_copy(2, y_peer), hid_copy(3, d_peer)]
    for copy in hid_copies:
        copy.start()
    hid_in[0] = hid[chip]

    loads[CHUNKS].wait()
    mlp = jnp.dot(hid[0], down[0:span, :], preferred_element_type=jnp.float32)
    for q in range(1, chips):
        mlp += jnp.dot(hid[q], down[q * span:(q + 1) * span, :], preferred_element_type=jnp.float32)
    for g in range(tp):
        piece = mlp[:, g * group:(g + 1) * group]
        part[g] = jnp.concatenate([piece[:half], piece[half:]], axis=1).astype(jnp.bfloat16)
    part_copies = [
        remote(part.at[lax.rem(me + k, tp)], part_in.at[k], part_send.at[k], part_recv.at[k], peers[k - 1])
        for k in range(1, tp)
    ]
    for copy in part_copies:
        copy.start()

    gain = gain_ref[...]
    gg = cot_ref[...].astype(jnp.float32) * gain
    for k in range(1, tp):
        lcb_arrival(k).wait_recv()
    packed = part[me].astype(jnp.float32)
    for k in range(1, tp):
        part_copies[k - 1].wait_recv()
        packed += part_in[k].astype(jnp.float32)
    summed = jnp.concatenate([packed[:, :group], packed[:, group:]], axis=0)
    linear = jnp.concatenate([lcb_in[t] for t in range(tp)], axis=0)
    mix = jnp.concatenate([summed, linear], axis=1)

    mean = jnp.sum(mix, axis=1, keepdims=True) * (1.0 / width)
    off = mix - mean
    dev = jnp.sum(off * off, axis=1, keepdims=True)
    first = jnp.sum(gg, axis=1, keepdims=True)
    second = jnp.sum(gg * off, axis=1, keepdims=True)
    lane = lax.broadcasted_iota(jnp.int32, (rows, 128), 1)
    table = jnp.where(lane == 0, mean, jnp.where(lane == 1, dev, jnp.where(lane == 2, first, second)))
    if rows < 128:
        table = jnp.concatenate([table, jnp.zeros((128 - rows, 128), jnp.float32)], axis=0)
    stat[...] = table.T[:8]
    stat_copies = [
        remote(stat, stat_in.at[k], stat_send.at[k], stat_recv.at[k], peers[k - 1]) for k in range(1, tp)
    ]
    for copy in stat_copies:
        copy.start()
    tables = [stat[...]]
    for k in range(1, tp):
        stat_copies[k - 1].wait_recv()
        tables.append(stat_in[k])
    full = float(tp * width)
    mean_all = sum(t[0:1] for t in tables) * (1.0 / tp)
    dev_all = sum(t[1:2] + (t[0:1] - mean_all) * (t[0:1] - mean_all) * float(width) for t in tables)
    first_all = sum(t[2:3] for t in tables) * (1.0 / full)
    rstd_all = 1.0 / jnp.sqrt(dev_all * (1.0 / full) + EPS)
    second_all = sum(t[3:4] + (t[0:1] - mean_all) * t[2:3] for t in tables) * rstd_all * (1.0 / full)
    back = jnp.concatenate(
        [mean_all, rstd_all, first_all, second_all, jnp.zeros((124, 128), jnp.float32)], axis=0
    ).T[:rows]
    mean_c, rstd_c, first_c, second_c = back[:, 0:1], back[:, 1:2], back[:, 2:3], back[:, 3:4]
    xhat = (mix - mean_c) * rstd_c
    grad = (gg[:, :group] - first_c - xhat[:, :group] * second_c) * rstd_c
    dmix[0, me] = jnp.concatenate([grad[:half], grad[half:]], axis=1).astype(jnp.bfloat16)

    def owner_at(k):
        return lax.rem(me + k, tp)

    def col_copy(k):
        return remote(dmix.at[0, me], dmix.at[0, me], col_send.at[k], col_recv.at[k], peers[k - 1])

    def col_arrival(k):
        ref = dmix.at[0, owner_at(k)]
        return remote(ref, ref, col_send.at[tp - k], col_recv.at[tp - k], peers[k - 1])

    def x_copy(k):
        return remote(dmix.at[0, owner_at(k)], dmix.at[1, owner_at(k)], x_send.at[k], x_recv.at[k], {"dp": x_peer})

    def y_copy(k):
        return remote(dmix.at[0, owner_at(k)], dmix.at[2, owner_at(k)], y_send.at[k], y_recv.at[k], {"dp": y_peer})

    def x_arrival(k):
        return remote(dmix.at[0, owner_at(k)], dmix.at[1, owner_at(k)], x_send.at[k], x_recv.at[k], {"dp": x_peer})

    def y_arrival(k):
        return remote(dmix.at[0, owner_at(k)], dmix.at[2, owner_at(k)], y_send.at[k], y_recv.at[k], {"dp": y_peer})

    def d_copy(k):
        slot, peer = (1, y_peer) if k % 2 == 0 else (2, x_peer)
        return remote(dmix.at[slot, owner_at(k)], dmix.at[3, owner_at(k)], d_send.at[k], d_recv.at[k], {"dp": peer})

    for k in range(1, tp):
        col_copy(k).start()
    x_copy(0).start()
    y_copy(0).start()
    res_ref[...] = (xhat * gain).astype(jnp.bfloat16)
    for copy in hid_copies:
        copy.wait_recv()
    for k in range(tp + 1):
        if 0 < k < tp:
            col_arrival(k).wait_recv()
            x_copy(k).start()
            y_copy(k).start()
        if k > 0:
            x_arrival(k - 1).wait_recv()
            y_arrival(k - 1).wait_recv()
            d_copy(k - 1).start()
    for k in range(tp):
        d_copy(k).wait_recv()

    across = (((0,), (0,)), ((), ()))
    low = jnp.concatenate([hid_in[s, :half] for s in range(chips)], axis=0)
    high = jnp.concatenate([hid_in[s, half:] for s in range(chips)], axis=0)
    columns = []
    for g in range(tp):
        block = jnp.concatenate([dmix[s, g] for s in range(chips)], axis=0)
        left = lax.dot_general(low, block, across, preferred_element_type=jnp.float32)
        right = lax.dot_general(high, block, across, preferred_element_type=jnp.float32)
        columns.append(left[:, :group] + right[:, group:])
    result = jnp.concatenate(columns, axis=1)
    mine = span // 2
    own = jnp.where(core == 0, result[:mine], result[mine:])
    half_out[...] = jnp.where(core == 0, result[mine:], result[:mine]).astype(jnp.bfloat16)
    c_copy = remote(half_out, half_in, c_send, c_recv, {"dp": c_peer})
    c_copy.start()

    for way in range(2):
        for d in range(tp - 1):
            @pl.when(sends(way, d))
            def _():
                for c in range(CHUNKS):
                    hop(way, d, c).wait_send()
    for copy in hid_copies + part_copies + stat_copies:
        copy.wait_send()
    for k in range(1, tp):
        lcb_copy(k).wait_send()
        col_copy(k).wait_send()
    for k in range(tp):
        x_copy(k).wait_send()
        y_copy(k).wait_send()
        d_copy(k).wait_send()
    c_copy.wait()
    grad_ref[...] = own + half_in[...].astype(jnp.float32)


def fused_device(dp, tp, embeddings, projection, compress, w_up, w_down, output_norm_gain, out_grad):
    samples = embeddings.shape[0]
    rows = samples * tp
    group = w_down.shape[1] // tp
    hidden = w_up.shape[1]
    pairs = jnp.einsum(
        "sef,fk->sek", embeddings, projection, preferred_element_type=jnp.float32
    ).astype(jnp.bfloat16)
    inter = jnp.einsum(
        "sek,sef->skf", pairs, embeddings, preferred_element_type=jnp.float32
    )
    center = inter - jnp.mean(inter, axis=(1, 2), keepdims=True)
    spread = jnp.mean(center * center, axis=(1, 2), keepdims=True)
    normed = (center / jnp.sqrt(spread + EPS)).astype(jnp.bfloat16)
    lcb = jnp.einsum(
        "sef,fj->sje", embeddings, compress, preferred_element_type=jnp.float32
    ).reshape(samples, tp, group).transpose(1, 0, 2)
    feats = w_up.shape[0] // (2 * CHUNKS)
    normed = normed.reshape(samples, CHUNKS, 2, feats).transpose(1, 2, 0, 3).reshape(CHUNKS, 2 * samples, feats)
    span = 2 * hidden // dp
    chips = dp // 2
    half = rows // 2
    width = 2 * group
    bf16, f32, dma = jnp.bfloat16, jnp.float32, pltpu.SemaphoreType.DMA
    vmem = pl.BlockSpec(memory_space=pltpu.VMEM)
    hbm = pl.BlockSpec(memory_space=pl.ANY)
    return pl.pallas_call(
        functools.partial(fused_kernel, dp, tp, samples, rows, group),
        out_shape=(
            jax.ShapeDtypeStruct((rows, width), bf16),
            jax.ShapeDtypeStruct((span // 2, w_down.shape[1]), f32),
        ),
        in_specs=[vmem, vmem, hbm, hbm, vmem, vmem],
        out_specs=(vmem, vmem),
        scratch_shapes=[
            pltpu.VMEM(w_up.shape, bf16),
            pltpu.VMEM(w_down.shape, bf16),
            pltpu.VMEM((CHUNKS, tp * 2 * samples, feats), bf16),
            pltpu.VMEM((tp, samples, group), f32),
            pltpu.VMEM((2, tp * 2 * samples, hidden), f32),
            pltpu.VMEM((chips, rows, span), bf16),
            pltpu.VMEM((chips, rows, span), bf16),
            pltpu.VMEM((tp, half, width), bf16),
            pltpu.VMEM((tp, half, width), bf16),
            pltpu.VMEM((8, 128), f32),
            pltpu.VMEM((tp, 8, 128), f32),
            pltpu.VMEM((chips, tp, half, width), bf16),
            pltpu.VMEM((span // 2, w_down.shape[1]), bf16),
            pltpu.VMEM((span // 2, w_down.shape[1]), bf16),
            dma((CHUNKS + 1,)),
            dma((2, tp, CHUNKS)), dma((2, tp, CHUNKS)),
            dma((tp,)), dma((tp,)),
            dma((4,)), dma((4,)),
            dma((tp,)), dma((tp,)),
            dma((tp,)), dma((tp,)),
            dma((tp,)), dma((tp,)),
            dma((tp,)), dma((tp,)),
            dma((tp,)), dma((tp,)),
            dma((tp,)), dma((tp,)),
            dma, dma,
        ],
        compiler_params=pltpu.CompilerParams(
            collective_id=0, has_side_effects=True, vmem_limit_bytes=48 * 1024 * 1024
        ),
        name="block",
    )(normed, lcb, w_up, w_down, output_norm_gain.reshape(1, width), out_grad)


def fits(dp, tp, args):
    embeddings, w_up, w_down = args[0], args[3], args[4]
    if dp != 8 or tp < 2 or embeddings.shape[0] % (dp * tp):
        return False
    samples = embeddings.shape[0] // (dp * tp)
    rows, group, hidden = samples * tp, w_down.shape[1] // tp, w_up.shape[1] // tp
    return (
        samples % 8 == 0 and rows % 32 == 0 and rows <= 128 and group % 64 == 0
        and hidden % (128 * dp) == 0 and w_up.shape[0] % (256 * CHUNKS) == 0
    )


def merged(value, axis, join):
    pieces = jax.tree.map(lambda part: lax.all_gather(part, axis), value)
    head = jax.tree.map(lambda part: part[0], pieces)
    tail = jax.tree.map(lambda part: part[1:], pieces)
    subtotal, _ = lax.scan(lambda subtotal, share: (join(subtotal, share), None), head, tail)
    return subtotal


def chan_merge(left, right):
    count_a, mean_a, dev_a = left
    count_b, mean_b, dev_b = right
    total = count_a + count_b
    delta = mean_b - mean_a
    row_average = mean_a + delta * (count_b / total)
    dev = dev_a + dev_b + delta * delta * (count_a * count_b / total)
    return (total, row_average, dev)


def alternate(mlp_part, lcb_part, groups):
    rows = mlp_part.shape[0]
    return jnp.concatenate(
        [mlp_part.reshape(rows, groups, -1), lcb_part.reshape(rows, groups, -1)], axis=2
    ).reshape(rows, -1)


def on_device(embeddings, projection, compress, w_up, w_down, output_norm_gain, out_grad):
    samples = embeddings.shape[0]
    pairs = jnp.einsum(
        "sef,fk->sek", embeddings, projection, preferred_element_type=jnp.float32
    ).astype(jnp.bfloat16)
    inter = jnp.einsum(
        "sek,sef->skf", pairs, embeddings, preferred_element_type=jnp.float32
    ).reshape(samples, -1)
    center = inter - jnp.mean(inter, axis=1, keepdims=True)
    spread = jnp.mean(center * center, axis=1, keepdims=True)
    normed = (center / jnp.sqrt(spread + 1e-05)).astype(jnp.bfloat16)
    lcb = jnp.einsum(
        "sef,fj->sje", embeddings, compress, preferred_element_type=jnp.float32
    ).reshape(samples, -1)
    hidden = jax.nn.gelu(
        jnp.dot(
            lax.all_gather(normed, "tp", axis=0, tiled=True),
            w_up,
            preferred_element_type=jnp.float32,
        ),
        approximate=True,
    ).astype(jnp.bfloat16)
    group_rows = hidden.shape[0]
    tp_count = lax.axis_size("tp")
    position = lax.axis_index("tp")
    mlp = jnp.dot(hidden, w_down, preferred_element_type=jnp.float32)
    mlp_width = mlp.shape[1]
    full_width = mlp_width + lcb.shape[1]
    width = full_width // tp_count
    placed = lax.dynamic_update_slice(
        jnp.zeros((group_rows, lcb.shape[1]), jnp.float32), lcb, (position * samples, jnp.int32(0))
    )
    term = alternate(mlp, placed, tp_count)
    mixed_rows = lax.psum_scatter(
        term.astype(jnp.bfloat16), "tp", scatter_dimension=1, tiled=True
    ).astype(jnp.float32)
    own_mean = jnp.mean(mixed_rows, axis=1)
    own_dev = jnp.sum((mixed_rows - own_mean[:, None]) ** 2, axis=1)
    own_count = jnp.full((), width, jnp.float32)
    total, row_average, dev = merged((own_count, own_mean, own_dev), "tp", chan_merge)
    inverse_deviation = 1.0 / jnp.sqrt(dev[:, None] / total + 1e-05)
    centered_rows = (mixed_rows - row_average[:, None]) * inverse_deviation
    block_result = (centered_rows * output_norm_gain).astype(jnp.bfloat16)
    scaled_rows = out_grad.astype(jnp.float32) * output_norm_gain
    sum_one, sum_two = lax.psum(
        (jnp.sum(scaled_rows, axis=1), jnp.sum(scaled_rows * centered_rows, axis=1)), "tp"
    )
    first_moment = (sum_one / full_width)[:, None]
    second_moment = (sum_two / full_width)[:, None]
    local_grad = (
        (scaled_rows - first_moment - centered_rows * second_moment) * inverse_deviation
    ).astype(jnp.bfloat16)
    mixed_gradient = lax.all_gather(local_grad, "tp", axis=1, tiled=True)
    group_mlp = mlp_width // tp_count
    mlp_grad = mixed_gradient.reshape(group_rows, tp_count, -1)[:, :, :group_mlp].reshape(
        group_rows, -1
    )
    grad_down = lax.psum_scatter(
        jnp.einsum("rh,rc->hc", hidden, mlp_grad, preferred_element_type=jnp.float32).astype(
            jnp.bfloat16
        ),
        "dp",
        scatter_dimension=0,
        tiled=True,
    ).astype(jnp.float32)
    return (block_result, grad_down)


def solution(mesh):
    dp, tp = mesh.shape["dp"], mesh.shape["tp"]

    def whole(*args):
        body = functools.partial(fused_device, dp, tp) if fits(dp, tp, args) else on_device
        return jax.shard_map(
            body,
            mesh=mesh,
            in_specs=(
                P(("dp", "tp"), None, None),
                P(),
                P(),
                P(None, "tp"),
                P("tp", None),
                P("tp"),
                P("dp", "tp"),
            ),
            out_specs=(P("dp", "tp"), P(("tp", "dp"), None)),
            check_vma=False,
        )(*args)

    return whole
```

```python
import functools

import jax
import jax.numpy as jnp
from jax import lax
from jax.experimental import pallas as pl
from jax.experimental.pallas import tpu as pltpu
from jax.sharding import PartitionSpec as P

CHUNKS = 4
EPS = 1e-05


def fused_kernel(
    dp, tp, samples, rows, group,
    emb_hbm, proj_ref, comp_ref, up_hbm, down_hbm, gain_ref, cot_ref,
    res_ref, grad_ref,
    emb, inter, linear_rows, lcb_ref, up, down, gathered, lcb_in, acc, hid, hid_in, part, part_in, stat, stat_in, dmix, half_out, half_in,
    emb_sem, load_sem, ag_send, ag_recv, lcb_send, lcb_recv, hid_send, hid_recv, part_send, part_recv,
    stat_send, stat_recv, col_send, col_recv, x_send, x_recv, y_send, y_recv, d_send, d_recv, c_send, c_recv,
):
    me = lax.axis_index("tp")
    ring = lax.axis_index("dp")
    core = lax.rem(ring, 2)
    east = lax.rem(ring // 2, 2)
    north = ring // 4
    x_peer = ring + 2 - 4 * east
    y_peer = ring + 4 - 8 * north
    d_peer = x_peer + 4 - 8 * north
    c_peer = ring + 1 - 2 * core
    chip = ring // 2
    half = rows // 2
    tall = 2 * samples
    feats = gathered.shape[2]
    rank, fields = proj_ref.shape
    width = 2 * group

    batch = emb_sem.shape[0]
    step = samples // batch
    emb_loads = [
        pltpu.make_async_copy(emb_hbm.at[pl.ds(b * step, step)], emb.at[pl.ds(b * step, step)], emb_sem.at[b])
        for b in range(batch)
    ]
    for load in emb_loads:
        load.start()
    loads = []
    for c in range(CHUNKS):
        piece = pl.ds(c * 2 * feats, 2 * feats)
        loads.append(pltpu.make_async_copy(up_hbm.at[piece], up.at[piece], load_sem.at[c]))
    loads.append(pltpu.make_async_copy(down_hbm, down, load_sem.at[CHUNKS]))
    for load in loads:
        load.start()

    order = [me]
    for k in range(1, tp):
        place = me * 0
        for t in range(tp):
            near = sorted(range(tp), key=lambda other: (abs(other - t), other))
            place = place + jnp.where(me == t, near[k], 0)
        order.append(place)
    peers = [{"tp": place} for place in order[1:]]
    others = [{"dp": x_peer}, {"dp": y_peer}, {"dp": d_peer}, {"dp": c_peer}]
    barrier = pltpu.get_barrier_semaphore()
    for peer in peers + others:
        pl.semaphore_signal(barrier, inc=1, device_id=peer, device_id_type=pl.DeviceIdType.MESH)

    spare = (-(rank + tp)) % 16
    strips = [(at, min(at + 128, group)) for at in range(0, group, 128)]
    head = jnp.concatenate(
        [proj_ref[...].astype(jnp.float32), comp_ref[...].astype(jnp.float32), jnp.zeros((spare, fields), jnp.float32)],
        axis=0,
    ).astype(jnp.bfloat16)
    for s in range(samples):
        if s % step == 0:
            emb_loads[s // step].wait()
        first = lax.dot_general(head, emb[s], (((1,), (1,)), ((), ())), preferred_element_type=jnp.float32)
        second = jnp.dot(first[:rank].astype(jnp.bfloat16), emb[s], preferred_element_type=jnp.float32)
        for h in range(fields // 128):
            inter[h, s * rank:(s + 1) * rank, :] = second[:, h * 128:(h + 1) * 128]
        for h, (at, end) in enumerate(strips):
            linear_rows[h, s * 8:(s + 1) * 8, 0:end - at] = first[rank:rank + 8, at:end]
    ranks = [
        jnp.concatenate([inter[h, pl.ds(k, samples, stride=rank), :] for h in range(fields // 128)], axis=1)
        for k in range(rank)
    ]
    count = float(rank * fields)
    center = jnp.sum(sum(ranks), axis=1, keepdims=True) * (1.0 / count)
    ranks = [value - center for value in ranks]
    spread = jnp.sum(sum(value * value for value in ranks), axis=1, keepdims=True) * (1.0 / count)
    scale = 1.0 / jnp.sqrt(spread + EPS)
    side_ranks = feats // fields
    for c in range(CHUNKS):
        for r in range(side_ranks):
            top = ranks[2 * c * side_ranks + r] * scale
            low = ranks[(2 * c + 1) * side_ranks + r] * scale
            gathered[c, pl.ds(pl.multiple_of(me * tall, tall), tall), r * fields:(r + 1) * fields] = (
                jnp.concatenate([top, low], axis=0).astype(jnp.bfloat16))
    pl.semaphore_wait(barrier, tp + 3)

    def remote(src, dst, send, recv, peer):
        return pltpu.make_async_remote_copy(
            src_ref=src, dst_ref=dst, send_sem=send, recv_sem=recv,
            device_id=peer, device_id_type=pl.DeviceIdType.MESH,
        )

    def block_rows(owner):
        return pl.ds(pl.multiple_of(owner * tall, tall), tall)

    def hop(way, d, c):
        step = 1 if way == 0 else -1
        owner = me - step * d
        dst = gathered.at[c, block_rows(owner)]
        return remote(dst, dst, ag_send.at[way, d, c], ag_recv.at[way, d + 1, c],
                      {"tp": lax.rem(me + step + tp, tp)})

    def arrival(way, d, c):
        step = 1 if way == 0 else -1
        owner = me - step * d
        dst = gathered.at[c, block_rows(owner)]
        return remote(dst, dst, ag_send.at[way, d, c], ag_recv.at[way, d, c],
                      {"tp": lax.rem(me + step + tp, tp)})

    def sends(way, d):
        return (me >= d) & (me < tp - 1) if way == 0 else (me < tp - d) & (me > 0)

    def gets(way, d):
        return me >= d if way == 0 else me < tp - d

    for way in range(2):
        @pl.when(sends(way, 0))
        def _():
            for c in range(CHUNKS):
                hop(way, 0, c).start()
    for j in range(tp):
        for h, (at, end) in enumerate(strips):
            lcb_ref[j, :, at:end] = linear_rows[h, pl.ds(j, samples, stride=8), :][:, :end - at]
    lcb_in[me] = lcb_ref[me]

    def lcb_copy(k):
        return remote(lcb_ref.at[order[k]], lcb_in.at[me], lcb_send.at[k], lcb_recv.at[me], peers[k - 1])

    def lcb_arrival(k):
        src = order[k]
        return remote(lcb_in.at[src], lcb_in.at[src], lcb_send.at[k], lcb_recv.at[src], peers[k - 1])

    for d in range(1, tp):
        if d == tp - 1:
            for k in range(1, tp):
                lcb_copy(k).start()
        for c in range(CHUNKS):
            for way in range(2):
                @pl.when(gets(way, d))
                def _():
                    arrival(way, d, c).wait_recv()
                if d < tp - 1:
                    @pl.when(sends(way, d))
                    def _():
                        hop(way, d, c).start()
            if d == tp - 1:
                loads[c].wait()
                for side in range(2):
                    term = jnp.dot(gathered[c], up[pl.ds((2 * c + side) * feats, feats), :],
                                   preferred_element_type=jnp.float32)
                    if c == 0:
                        acc[side] = term
                    else:
                        acc[side] += term

    for t in range(tp):
        total = acc[0, t * tall:t * tall + samples] + acc[1, t * tall + samples:(t + 1) * tall]
        acc[0, t * samples:(t + 1) * samples] = total
    chips = dp // 2
    span = hid.shape[2]
    for q in range(chips):
        hid[q] = jax.nn.gelu(acc[0, :rows, q * span:(q + 1) * span], approximate=True).astype(jnp.bfloat16)

    def hid_copy(slot, peer):
        return remote(hid.at[peer // 2], hid_in.at[slot], hid_send.at[slot], hid_recv.at[slot], {"dp": peer})

    hid_copies = [hid_copy(1, x_peer), hid_copy(2, y_peer), hid_copy(3, d_peer)]
    for copy in hid_copies:
        copy.start()
    hid_in[0] = hid[chip]

    loads[CHUNKS].wait()
    mlp = jnp.dot(hid[0], down[0:span, :], preferred_element_type=jnp.float32)
    for q in range(1, chips):
        mlp += jnp.dot(hid[q], down[q * span:(q + 1) * span, :], preferred_element_type=jnp.float32)
    for g in range(tp):
        piece = mlp[:, g * group:(g + 1) * group]
        part[g] = jnp.concatenate([piece[:half], piece[half:]], axis=1).astype(jnp.bfloat16)
    def exchange(source, landing, send, recv):
        outs = [remote(source(order[k]), landing.at[me], send.at[k], recv.at[me], peers[k - 1]) for k in range(1, tp)]
        ins = [
            remote(landing.at[order[k]], landing.at[order[k]], send.at[k], recv.at[order[k]], peers[k - 1])
            for k in range(1, tp)
        ]
        for copy in reversed(outs):
            copy.start()
        return outs, ins

    part_copies, part_ins = exchange(lambda place: part.at[place], part_in, part_send, part_recv)

    gain = gain_ref[...]
    gg = cot_ref[...].astype(jnp.float32) * gain
    for k in range(1, tp):
        lcb_arrival(k).wait_recv()
    packed = part[me].astype(jnp.float32)
    for k in range(1, tp):
        part_ins[k - 1].wait_recv()
        packed += part_in[order[k]].astype(jnp.float32)
    summed = jnp.concatenate([packed[:, :group], packed[:, group:]], axis=0)
    linear = jnp.concatenate([lcb_in[t] for t in range(tp)], axis=0)
    mix = jnp.concatenate([summed, linear], axis=1)

    mean = jnp.sum(mix, axis=1, keepdims=True) * (1.0 / width)
    off = mix - mean
    dev = jnp.sum(off * off, axis=1, keepdims=True)
    first = jnp.sum(gg, axis=1, keepdims=True)
    second = jnp.sum(gg * off, axis=1, keepdims=True)
    lane = lax.broadcasted_iota(jnp.int32, (rows, 128), 1)
    table = jnp.where(lane == 0, mean, jnp.where(lane == 1, dev, jnp.where(lane == 2, first, second)))
    if rows < 128:
        table = jnp.concatenate([table, jnp.zeros((128 - rows, 128), jnp.float32)], axis=0)
    stat[...] = table.T[:8]
    stat_copies, stat_ins = exchange(lambda place: stat, stat_in, stat_send, stat_recv)
    tables = [stat[...]]
    for k in range(1, tp):
        stat_ins[k - 1].wait_recv()
        tables.append(stat_in[order[k]])
    full = float(tp * width)
    mean_all = sum(t[0:1] for t in tables) * (1.0 / tp)
    dev_all = sum(t[1:2] + (t[0:1] - mean_all) * (t[0:1] - mean_all) * float(width) for t in tables)
    first_all = sum(t[2:3] for t in tables) * (1.0 / full)
    rstd_all = 1.0 / jnp.sqrt(dev_all * (1.0 / full) + EPS)
    second_all = sum(t[3:4] + (t[0:1] - mean_all) * t[2:3] for t in tables) * rstd_all * (1.0 / full)
    back = jnp.concatenate(
        [mean_all, rstd_all, first_all, second_all, jnp.zeros((124, 128), jnp.float32)], axis=0
    ).T[:rows]
    mean_c, rstd_c, first_c, second_c = back[:, 0:1], back[:, 1:2], back[:, 2:3], back[:, 3:4]
    xhat = (mix - mean_c) * rstd_c
    grad = (gg[:, :group] - first_c - xhat[:, :group] * second_c) * rstd_c
    dmix[0, me] = jnp.concatenate([grad[:half], grad[half:]], axis=1).astype(jnp.bfloat16)

    def owner_at(k):
        return order[k]

    def x_copy(k):
        return remote(dmix.at[0, owner_at(k)], dmix.at[1, owner_at(k)], x_send.at[k], x_recv.at[k], {"dp": x_peer})

    def y_copy(k):
        return remote(dmix.at[0, owner_at(k)], dmix.at[2, owner_at(k)], y_send.at[k], y_recv.at[k], {"dp": y_peer})

    def x_arrival(k):
        return remote(dmix.at[0, owner_at(k)], dmix.at[1, owner_at(k)], x_send.at[k], x_recv.at[k], {"dp": x_peer})

    def y_arrival(k):
        return remote(dmix.at[0, owner_at(k)], dmix.at[2, owner_at(k)], y_send.at[k], y_recv.at[k], {"dp": y_peer})

    def d_copy(k):
        slot, peer = (1, y_peer) if k % 2 == 0 else (2, x_peer)
        return remote(dmix.at[slot, owner_at(k)], dmix.at[3, owner_at(k)], d_send.at[k], d_recv.at[k], {"dp": peer})

    col_copies, col_ins = exchange(lambda place: dmix.at[0, me], dmix.at[0], col_send, col_recv)
    x_copy(0).start()
    y_copy(0).start()
    res_ref[...] = (xhat * gain).astype(jnp.bfloat16)
    for copy in hid_copies:
        copy.wait_recv()
    for k in range(tp + 1):
        if 0 < k < tp:
            col_ins[k - 1].wait_recv()
            x_copy(k).start()
            y_copy(k).start()
        if k > 0:
            x_arrival(k - 1).wait_recv()
            y_arrival(k - 1).wait_recv()
            d_copy(k - 1).start()
    for k in range(tp):
        d_copy(k).wait_recv()

    across = (((0,), (0,)), ((), ()))
    low = jnp.concatenate([hid_in[s, :half] for s in range(chips)], axis=0)
    high = jnp.concatenate([hid_in[s, half:] for s in range(chips)], axis=0)
    columns = []
    for g in range(tp):
        block = jnp.concatenate([dmix[s, g] for s in range(chips)], axis=0)
        left = lax.dot_general(low, block, across, preferred_element_type=jnp.float32)
        right = lax.dot_general(high, block, across, preferred_element_type=jnp.float32)
        columns.append(left[:, :group] + right[:, group:])
    result = jnp.concatenate(columns, axis=1)
    mine = span // 2
    own = jnp.where(core == 0, result[:mine], result[mine:])
    half_out[...] = jnp.where(core == 0, result[mine:], result[:mine]).astype(jnp.bfloat16)
    c_copy = remote(half_out, half_in, c_send, c_recv, {"dp": c_peer})
    c_copy.start()

    for way in range(2):
        for d in range(tp - 1):
            @pl.when(sends(way, d))
            def _():
                for c in range(CHUNKS):
                    hop(way, d, c).wait_send()
    for copy in hid_copies + part_copies + stat_copies + col_copies:
        copy.wait_send()
    for k in range(1, tp):
        lcb_copy(k).wait_send()
    for k in range(tp):
        x_copy(k).wait_send()
        y_copy(k).wait_send()
        d_copy(k).wait_send()
    c_copy.wait()
    grad_ref[...] = own + half_in[...].astype(jnp.float32)


def fused_device(dp, tp, embeddings, projection, compress, w_up, w_down, output_norm_gain, out_grad):
    samples = embeddings.shape[0]
    rows = samples * tp
    group = w_down.shape[1] // tp
    hidden = w_up.shape[1]
    feats = w_up.shape[0] // (2 * CHUNKS)
    span = 2 * hidden // dp
    chips = dp // 2
    half = rows // 2
    width = 2 * group
    bf16, f32, dma = jnp.bfloat16, jnp.float32, pltpu.SemaphoreType.DMA
    vmem = pl.BlockSpec(memory_space=pltpu.VMEM)
    hbm = pl.BlockSpec(memory_space=pltpu.HBM)
    return pl.pallas_call(
        functools.partial(fused_kernel, dp, tp, samples, rows, group),
        out_shape=(
            jax.ShapeDtypeStruct((rows, width), bf16),
            jax.ShapeDtypeStruct((span // 2, w_down.shape[1]), f32),
        ),
        in_specs=[hbm, vmem, vmem, hbm, hbm, vmem, vmem],
        out_specs=(vmem, vmem),
        scratch_shapes=[
            pltpu.VMEM(embeddings.shape, bf16),
            pltpu.VMEM((embeddings.shape[2] // 128, samples * projection.shape[1], 128), f32),
            pltpu.VMEM((pl.cdiv(group, 128), samples * 8, 128), f32),
            pltpu.VMEM((tp, samples, group), f32),
            pltpu.VMEM(w_up.shape, bf16),
            pltpu.VMEM(w_down.shape, bf16),
            pltpu.VMEM((CHUNKS, tp * 2 * samples, feats), bf16),
            pltpu.VMEM((tp, samples, group), f32),
            pltpu.VMEM((2, tp * 2 * samples, hidden), f32),
            pltpu.VMEM((chips, rows, span), bf16),
            pltpu.VMEM((chips, rows, span), bf16),
            pltpu.VMEM((tp, half, width), bf16),
            pltpu.VMEM((tp, half, width), bf16),
            pltpu.VMEM((8, 128), f32),
            pltpu.VMEM((tp, 8, 128), f32),
            pltpu.VMEM((chips, tp, half, width), bf16),
            pltpu.VMEM((span // 2, w_down.shape[1]), bf16),
            pltpu.VMEM((span // 2, w_down.shape[1]), bf16),
            dma((3 if samples % 3 == 0 else 1,)),
            dma((CHUNKS + 1,)),
            dma((2, tp, CHUNKS)), dma((2, tp, CHUNKS)),
            dma((tp,)), dma((tp,)),
            dma((4,)), dma((4,)),
            dma((tp,)), dma((tp,)),
            dma((tp,)), dma((tp,)),
            dma((tp,)), dma((tp,)),
            dma((tp,)), dma((tp,)),
            dma((tp,)), dma((tp,)),
            dma((tp,)), dma((tp,)),
            dma, dma,
        ],
        compiler_params=pltpu.CompilerParams(
            collective_id=0, has_side_effects=True, vmem_limit_bytes=65_800_000
        ),
        name="block",
    )(embeddings, projection.T, compress.T, w_up, w_down, output_norm_gain.reshape(1, width), out_grad)


def fits(dp, tp, args):
    embeddings, projection, compress, w_up, w_down = args[:5]
    if dp != 8 or tp < 2 or embeddings.shape[0] % (dp * tp):
        return False
    samples = embeddings.shape[0] // (dp * tp)
    rows, group, hidden = samples * tp, w_down.shape[1] // tp, w_up.shape[1] // tp
    return (
        compress.shape[1] == tp and embeddings.shape[1] == w_down.shape[1] // tp and tp <= 8
        and projection.shape[1] % (2 * CHUNKS) == 0 and projection.shape[1] % 16 == 0 and embeddings.shape[2] % 128 == 0
        and samples % 8 == 0 and rows % 32 == 0 and rows <= 128 and group % 64 == 0
        and hidden % (128 * dp) == 0 and w_up.shape[0] % (256 * CHUNKS) == 0
    )


def merged(value, axis, join):
    pieces = jax.tree.map(lambda part: lax.all_gather(part, axis), value)
    head = jax.tree.map(lambda part: part[0], pieces)
    tail = jax.tree.map(lambda part: part[1:], pieces)
    subtotal, _ = lax.scan(lambda subtotal, share: (join(subtotal, share), None), head, tail)
    return subtotal


def chan_merge(left, right):
    count_a, mean_a, dev_a = left
    count_b, mean_b, dev_b = right
    total = count_a + count_b
    delta = mean_b - mean_a
    row_average = mean_a + delta * (count_b / total)
    dev = dev_a + dev_b + delta * delta * (count_a * count_b / total)
    return (total, row_average, dev)


def alternate(mlp_part, lcb_part, groups):
    rows = mlp_part.shape[0]
    return jnp.concatenate(
        [mlp_part.reshape(rows, groups, -1), lcb_part.reshape(rows, groups, -1)], axis=2
    ).reshape(rows, -1)


def on_device(embeddings, projection, compress, w_up, w_down, output_norm_gain, out_grad):
    samples = embeddings.shape[0]
    pairs = jnp.einsum(
        "sef,fk->sek", embeddings, projection, preferred_element_type=jnp.float32
    ).astype(jnp.bfloat16)
    inter = jnp.einsum(
        "sek,sef->skf", pairs, embeddings, preferred_element_type=jnp.float32
    ).reshape(samples, -1)
    center = inter - jnp.mean(inter, axis=1, keepdims=True)
    spread = jnp.mean(center * center, axis=1, keepdims=True)
    normed = (center / jnp.sqrt(spread + 1e-05)).astype(jnp.bfloat16)
    lcb = jnp.einsum(
        "sef,fj->sje", embeddings, compress, preferred_element_type=jnp.float32
    ).reshape(samples, -1)
    hidden = jax.nn.gelu(
        jnp.dot(
            lax.all_gather(normed, "tp", axis=0, tiled=True),
            w_up,
            preferred_element_type=jnp.float32,
        ),
        approximate=True,
    ).astype(jnp.bfloat16)
    group_rows = hidden.shape[0]
    tp_count = lax.axis_size("tp")
    position = lax.axis_index("tp")
    mlp = jnp.dot(hidden, w_down, preferred_element_type=jnp.float32)
    mlp_width = mlp.shape[1]
    full_width = mlp_width + lcb.shape[1]
    width = full_width // tp_count
    placed = lax.dynamic_update_slice(
        jnp.zeros((group_rows, lcb.shape[1]), jnp.float32), lcb, (position * samples, jnp.int32(0))
    )
    term = alternate(mlp, placed, tp_count)
    mixed_rows = lax.psum_scatter(
        term.astype(jnp.bfloat16), "tp", scatter_dimension=1, tiled=True
    ).astype(jnp.float32)
    own_mean = jnp.mean(mixed_rows, axis=1)
    own_dev = jnp.sum((mixed_rows - own_mean[:, None]) ** 2, axis=1)
    own_count = jnp.full((), width, jnp.float32)
    total, row_average, dev = merged((own_count, own_mean, own_dev), "tp", chan_merge)
    inverse_deviation = 1.0 / jnp.sqrt(dev[:, None] / total + 1e-05)
    centered_rows = (mixed_rows - row_average[:, None]) * inverse_deviation
    block_result = (centered_rows * output_norm_gain).astype(jnp.bfloat16)
    scaled_rows = out_grad.astype(jnp.float32) * output_norm_gain
    sum_one, sum_two = lax.psum(
        (jnp.sum(scaled_rows, axis=1), jnp.sum(scaled_rows * centered_rows, axis=1)), "tp"
    )
    first_moment = (sum_one / full_width)[:, None]
    second_moment = (sum_two / full_width)[:, None]
    local_grad = (
        (scaled_rows - first_moment - centered_rows * second_moment) * inverse_deviation
    ).astype(jnp.bfloat16)
    mixed_gradient = lax.all_gather(local_grad, "tp", axis=1, tiled=True)
    group_mlp = mlp_width // tp_count
    mlp_grad = mixed_gradient.reshape(group_rows, tp_count, -1)[:, :, :group_mlp].reshape(
        group_rows, -1
    )
    grad_down = lax.psum_scatter(
        jnp.einsum("rh,rc->hc", hidden, mlp_grad, preferred_element_type=jnp.float32).astype(
            jnp.bfloat16
        ),
        "dp",
        scatter_dimension=0,
        tiled=True,
    ).astype(jnp.float32)
    return (block_result, grad_down)


def solution(mesh):
    dp, tp = mesh.shape["dp"], mesh.shape["tp"]

    def whole(*args):
        body = functools.partial(fused_device, dp, tp) if fits(dp, tp, args) else on_device
        return jax.shard_map(
            body,
            mesh=mesh,
            in_specs=(
                P(("dp", "tp"), None, None),
                P(),
                P(),
                P(None, "tp"),
                P("tp", None),
                P("tp"),
                P("dp", "tp"),
            ),
            out_specs=(P("dp", "tp"), P(("tp", "dp"), None)),
            check_vma=False,
        )(*args)

    return whole
```

```python
import functools

import jax
import jax.numpy as jnp
from jax import lax
from jax.experimental import pallas as pl
from jax.experimental.pallas import tpu as pltpu
from jax.sharding import PartitionSpec as P

CHUNKS = 4
EPS = 1e-05


def fused_kernel(
    dp, tp, samples, rows, group,
    norm_ref, lcb_ref, up_hbm, down_hbm, gain_ref, cot_ref,
    res_ref, grad_ref,
    up, down, gathered, lcb_in, acc, hid, hid_in, part, part_in, stat, stat_in, dmix, half_out, half_in,
    load_sem, ag_send, ag_recv, lcb_send, lcb_recv, hid_send, hid_recv, part_send, part_recv,
    stat_send, stat_recv, col_send, col_recv, x_send, x_recv, y_send, y_recv, d_send, d_recv, c_send, c_recv,
):
    me = lax.axis_index("tp")
    ring = lax.axis_index("dp")
    core = lax.rem(ring, 2)
    east = lax.rem(ring // 2, 2)
    north = ring // 4
    x_peer = ring + 2 - 4 * east
    y_peer = ring + 4 - 8 * north
    d_peer = x_peer + 4 - 8 * north
    c_peer = ring + 1 - 2 * core
    chip = ring // 2
    half = rows // 2
    tall = 2 * samples
    feats = norm_ref.shape[2]
    width = 2 * group

    loads = []
    for c in range(CHUNKS):
        piece = pl.ds(c * 2 * feats, 2 * feats)
        loads.append(pltpu.make_async_copy(up_hbm.at[piece], up.at[piece], load_sem.at[c]))
    loads.append(pltpu.make_async_copy(down_hbm, down, load_sem.at[CHUNKS]))
    for load in loads:
        load.start()

    order = [me]
    for k in range(1, tp):
        place = me * 0
        for t in range(tp):
            near = sorted(range(tp), key=lambda other: (abs(other - t), other))
            place = place + jnp.where(me == t, near[k], 0)
        order.append(place)
    peers = [{"tp": place} for place in order[1:]]
    others = [{"dp": x_peer}, {"dp": y_peer}, {"dp": d_peer}, {"dp": c_peer}]
    barrier = pltpu.get_barrier_semaphore()
    for peer in peers + others:
        pl.semaphore_signal(barrier, inc=1, device_id=peer, device_id_type=pl.DeviceIdType.MESH)
    pl.semaphore_wait(barrier, tp + 3)

    def remote(src, dst, send, recv, peer):
        return pltpu.make_async_remote_copy(
            src_ref=src, dst_ref=dst, send_sem=send, recv_sem=recv,
            device_id=peer, device_id_type=pl.DeviceIdType.MESH,
        )

    def block_rows(owner):
        return pl.ds(pl.multiple_of(owner * tall, tall), tall)

    def hop(way, d, c):
        step = 1 if way == 0 else -1
        owner = me - step * d
        dst = gathered.at[c, block_rows(owner)]
        src = norm_ref.at[c] if d == 0 else dst
        return remote(src, dst, ag_send.at[way, d, c], ag_recv.at[way, d + 1, c],
                      {"tp": lax.rem(me + step + tp, tp)})

    def arrival(way, d, c):
        step = 1 if way == 0 else -1
        owner = me - step * d
        dst = gathered.at[c, block_rows(owner)]
        return remote(dst, dst, ag_send.at[way, d, c], ag_recv.at[way, d, c],
                      {"tp": lax.rem(me + step + tp, tp)})

    def sends(way, d):
        return (me >= d) & (me < tp - 1) if way == 0 else (me < tp - d) & (me > 0)

    def gets(way, d):
        return me >= d if way == 0 else me < tp - d

    for way in range(2):
        @pl.when(sends(way, 0))
        def _():
            for c in range(CHUNKS):
                hop(way, 0, c).start()
    for c in range(CHUNKS):
        gathered[c, block_rows(me)] = norm_ref[c]
    lcb_in[me] = lcb_ref[me]

    def lcb_copy(k):
        return remote(lcb_ref.at[order[k]], lcb_in.at[me], lcb_send.at[k], lcb_recv.at[me], peers[k - 1])

    def lcb_arrival(k):
        src = order[k]
        return remote(lcb_in.at[src], lcb_in.at[src], lcb_send.at[k], lcb_recv.at[src], peers[k - 1])

    for d in range(1, tp):
        if d == tp - 1:
            for k in range(1, tp):
                lcb_copy(k).start()
        for c in range(CHUNKS):
            for way in range(2):
                @pl.when(gets(way, d))
                def _():
                    arrival(way, d, c).wait_recv()
                if d < tp - 1:
                    @pl.when(sends(way, d))
                    def _():
                        hop(way, d, c).start()
            if d == tp - 1:
                loads[c].wait()
                for side in range(2):
                    term = jnp.dot(gathered[c], up[pl.ds((2 * c + side) * feats, feats), :],
                                   preferred_element_type=jnp.float32)
                    if c == 0:
                        acc[side] = term
                    else:
                        acc[side] += term

    for t in range(tp):
        total = acc[0, t * tall:t * tall + samples] + acc[1, t * tall + samples:(t + 1) * tall]
        acc[0, t * samples:(t + 1) * samples] = total
    chips = dp // 2
    span = hid.shape[2]
    for q in range(chips):
        hid[q] = jax.nn.gelu(acc[0, :rows, q * span:(q + 1) * span], approximate=True).astype(jnp.bfloat16)

    def hid_copy(slot, peer):
        return remote(hid.at[peer // 2], hid_in.at[slot], hid_send.at[slot], hid_recv.at[slot], {"dp": peer})

    hid_copies = [hid_copy(1, x_peer), hid_copy(2, y_peer), hid_copy(3, d_peer)]
    for copy in hid_copies:
        copy.start()
    hid_in[0] = hid[chip]

    loads[CHUNKS].wait()
    mlp = jnp.dot(hid[0], down[0:span, :], preferred_element_type=jnp.float32)
    for q in range(1, chips):
        mlp += jnp.dot(hid[q], down[q * span:(q + 1) * span, :], preferred_element_type=jnp.float32)
    for g in range(tp):
        piece = mlp[:, g * group:(g + 1) * group]
        part[g] = jnp.concatenate([piece[:half], piece[half:]], axis=1).astype(jnp.bfloat16)
    def exchange(source, landing, send, recv):
        outs = [remote(source(order[k]), landing.at[me], send.at[k], recv.at[me], peers[k - 1]) for k in range(1, tp)]
        ins = [
            remote(landing.at[order[k]], landing.at[order[k]], send.at[k], recv.at[order[k]], peers[k - 1])
            for k in range(1, tp)
        ]
        for copy in reversed(outs):
            copy.start()
        return outs, ins

    part_copies, part_ins = exchange(lambda place: part.at[place], part_in, part_send, part_recv)

    gain = gain_ref[...]
    gg = cot_ref[...].astype(jnp.float32) * gain
    for k in range(1, tp):
        lcb_arrival(k).wait_recv()
    packed = part[me].astype(jnp.float32)
    for k in range(1, tp):
        part_ins[k - 1].wait_recv()
        packed += part_in[order[k]].astype(jnp.float32)
    summed = jnp.concatenate([packed[:, :group], packed[:, group:]], axis=0)
    linear = jnp.concatenate([lcb_in[t] for t in range(tp)], axis=0)
    mix = jnp.concatenate([summed, linear], axis=1)

    mean = jnp.sum(mix, axis=1, keepdims=True) * (1.0 / width)
    off = mix - mean
    dev = jnp.sum(off * off, axis=1, keepdims=True)
    first = jnp.sum(gg, axis=1, keepdims=True)
    second = jnp.sum(gg * off, axis=1, keepdims=True)
    lane = lax.broadcasted_iota(jnp.int32, (rows, 128), 1)
    table = jnp.where(lane == 0, mean, jnp.where(lane == 1, dev, jnp.where(lane == 2, first, second)))
    if rows < 128:
        table = jnp.concatenate([table, jnp.zeros((128 - rows, 128), jnp.float32)], axis=0)
    stat[...] = table.T[:8]
    stat_copies, stat_ins = exchange(lambda place: stat, stat_in, stat_send, stat_recv)
    tables = [stat[...]]
    for k in range(1, tp):
        stat_ins[k - 1].wait_recv()
        tables.append(stat_in[order[k]])
    full = float(tp * width)
    mean_all = sum(t[0:1] for t in tables) * (1.0 / tp)
    dev_all = sum(t[1:2] + (t[0:1] - mean_all) * (t[0:1] - mean_all) * float(width) for t in tables)
    first_all = sum(t[2:3] for t in tables) * (1.0 / full)
    rstd_all = 1.0 / jnp.sqrt(dev_all * (1.0 / full) + EPS)
    second_all = sum(t[3:4] + (t[0:1] - mean_all) * t[2:3] for t in tables) * rstd_all * (1.0 / full)
    back = jnp.concatenate(
        [mean_all, rstd_all, first_all, second_all, jnp.zeros((124, 128), jnp.float32)], axis=0
    ).T[:rows]
    mean_c, rstd_c, first_c, second_c = back[:, 0:1], back[:, 1:2], back[:, 2:3], back[:, 3:4]
    xhat = (mix - mean_c) * rstd_c
    grad = (gg[:, :group] - first_c - xhat[:, :group] * second_c) * rstd_c
    dmix[0, me] = jnp.concatenate([grad[:half], grad[half:]], axis=1).astype(jnp.bfloat16)

    def owner_at(k):
        return order[k]

    def x_copy(k):
        return remote(dmix.at[0, owner_at(k)], dmix.at[1, owner_at(k)], x_send.at[k], x_recv.at[k], {"dp": x_peer})

    def y_copy(k):
        return remote(dmix.at[0, owner_at(k)], dmix.at[2, owner_at(k)], y_send.at[k], y_recv.at[k], {"dp": y_peer})

    def x_arrival(k):
        return remote(dmix.at[0, owner_at(k)], dmix.at[1, owner_at(k)], x_send.at[k], x_recv.at[k], {"dp": x_peer})

    def y_arrival(k):
        return remote(dmix.at[0, owner_at(k)], dmix.at[2, owner_at(k)], y_send.at[k], y_recv.at[k], {"dp": y_peer})

    def d_copy(k):
        slot, peer = (1, y_peer) if k % 2 == 0 else (2, x_peer)
        return remote(dmix.at[slot, owner_at(k)], dmix.at[3, owner_at(k)], d_send.at[k], d_recv.at[k], {"dp": peer})

    col_copies, col_ins = exchange(lambda place: dmix.at[0, me], dmix.at[0], col_send, col_recv)
    x_copy(0).start()
    y_copy(0).start()
    res_ref[...] = (xhat * gain).astype(jnp.bfloat16)
    for copy in hid_copies:
        copy.wait_recv()
    for k in range(tp + 1):
        if 0 < k < tp:
            col_ins[k - 1].wait_recv()
            x_copy(k).start()
            y_copy(k).start()
        if k > 0:
            x_arrival(k - 1).wait_recv()
            y_arrival(k - 1).wait_recv()
            d_copy(k - 1).start()
    for k in range(tp):
        d_copy(k).wait_recv()

    across = (((0,), (0,)), ((), ()))
    low = jnp.concatenate([hid_in[s, :half] for s in range(chips)], axis=0)
    high = jnp.concatenate([hid_in[s, half:] for s in range(chips)], axis=0)
    columns = []
    for g in range(tp):
        block = jnp.concatenate([dmix[s, g] for s in range(chips)], axis=0)
        left = lax.dot_general(low, block, across, preferred_element_type=jnp.float32)
        right = lax.dot_general(high, block, across, preferred_element_type=jnp.float32)
        columns.append(left[:, :group] + right[:, group:])
    result = jnp.concatenate(columns, axis=1)
    mine = span // 2
    own = jnp.where(core == 0, result[:mine], result[mine:])
    half_out[...] = jnp.where(core == 0, result[mine:], result[:mine]).astype(jnp.bfloat16)
    c_copy = remote(half_out, half_in, c_send, c_recv, {"dp": c_peer})
    c_copy.start()

    for way in range(2):
        for d in range(tp - 1):
            @pl.when(sends(way, d))
            def _():
                for c in range(CHUNKS):
                    hop(way, d, c).wait_send()
    for copy in hid_copies + part_copies + stat_copies + col_copies:
        copy.wait_send()
    for k in range(1, tp):
        lcb_copy(k).wait_send()
    for k in range(tp):
        x_copy(k).wait_send()
        y_copy(k).wait_send()
        d_copy(k).wait_send()
    c_copy.wait()
    grad_ref[...] = own + half_in[...].astype(jnp.float32)


def fused_device(dp, tp, embeddings, projection, compress, w_up, w_down, output_norm_gain, out_grad):
    samples = embeddings.shape[0]
    rows = samples * tp
    group = w_down.shape[1] // tp
    hidden = w_up.shape[1]
    pairs = jnp.einsum(
        "sef,fk->sek", embeddings, projection, preferred_element_type=jnp.float32
    ).astype(jnp.bfloat16)
    inter = jnp.einsum(
        "sek,sef->skf", pairs, embeddings, preferred_element_type=jnp.float32
    )
    center = inter - jnp.mean(inter, axis=(1, 2), keepdims=True)
    spread = jnp.mean(center * center, axis=(1, 2), keepdims=True)
    normed = (center / jnp.sqrt(spread + EPS)).astype(jnp.bfloat16)
    lcb = jnp.einsum(
        "sef,fj->sje", embeddings, compress, preferred_element_type=jnp.float32
    ).reshape(samples, tp, group).transpose(1, 0, 2)
    feats = w_up.shape[0] // (2 * CHUNKS)
    normed = normed.reshape(samples, CHUNKS, 2, feats).transpose(1, 2, 0, 3).reshape(CHUNKS, 2 * samples, feats)
    span = 2 * hidden // dp
    chips = dp // 2
    half = rows // 2
    width = 2 * group
    bf16, f32, dma = jnp.bfloat16, jnp.float32, pltpu.SemaphoreType.DMA
    vmem = pl.BlockSpec(memory_space=pltpu.VMEM)
    hbm = pl.BlockSpec(memory_space=pl.ANY)
    return pl.pallas_call(
        functools.partial(fused_kernel, dp, tp, samples, rows, group),
        out_shape=(
            jax.ShapeDtypeStruct((rows, width), bf16),
            jax.ShapeDtypeStruct((span // 2, w_down.shape[1]), f32),
        ),
        in_specs=[vmem, vmem, hbm, hbm, vmem, vmem],
        out_specs=(vmem, vmem),
        scratch_shapes=[
            pltpu.VMEM(w_up.shape, bf16),
            pltpu.VMEM(w_down.shape, bf16),
            pltpu.VMEM((CHUNKS, tp * 2 * samples, feats), bf16),
            pltpu.VMEM((tp, samples, group), f32),
            pltpu.VMEM((2, tp * 2 * samples, hidden), f32),
            pltpu.VMEM((chips, rows, span), bf16),
            pltpu.VMEM((chips, rows, span), bf16),
            pltpu.VMEM((tp, half, width), bf16),
            pltpu.VMEM((tp, half, width), bf16),
            pltpu.VMEM((8, 128), f32),
            pltpu.VMEM((tp, 8, 128), f32),
            pltpu.VMEM((chips, tp, half, width), bf16),
            pltpu.VMEM((span // 2, w_down.shape[1]), bf16),
            pltpu.VMEM((span // 2, w_down.shape[1]), bf16),
            dma((CHUNKS + 1,)),
            dma((2, tp, CHUNKS)), dma((2, tp, CHUNKS)),
            dma((tp,)), dma((tp,)),
            dma((4,)), dma((4,)),
            dma((tp,)), dma((tp,)),
            dma((tp,)), dma((tp,)),
            dma((tp,)), dma((tp,)),
            dma((tp,)), dma((tp,)),
            dma((tp,)), dma((tp,)),
            dma((tp,)), dma((tp,)),
            dma, dma,
        ],
        compiler_params=pltpu.CompilerParams(
            collective_id=0, has_side_effects=True, vmem_limit_bytes=48 * 1024 * 1024
        ),
        name="block",
    )(normed, lcb, w_up, w_down, output_norm_gain.reshape(1, width), out_grad)


def fits(dp, tp, args):
    embeddings, w_up, w_down = args[0], args[3], args[4]
    if dp != 8 or tp < 2 or embeddings.shape[0] % (dp * tp):
        return False
    samples = embeddings.shape[0] // (dp * tp)
    rows, group, hidden = samples * tp, w_down.shape[1] // tp, w_up.shape[1] // tp
    return (
        samples % 8 == 0 and rows % 32 == 0 and rows <= 128 and group % 64 == 0
        and hidden % (128 * dp) == 0 and w_up.shape[0] % (256 * CHUNKS) == 0
    )


def merged(value, axis, join):
    pieces = jax.tree.map(lambda part: lax.all_gather(part, axis), value)
    head = jax.tree.map(lambda part: part[0], pieces)
    tail = jax.tree.map(lambda part: part[1:], pieces)
    subtotal, _ = lax.scan(lambda subtotal, share: (join(subtotal, share), None), head, tail)
    return subtotal


def chan_merge(left, right):
    count_a, mean_a, dev_a = left
    count_b, mean_b, dev_b = right
    total = count_a + count_b
    delta = mean_b - mean_a
    row_average = mean_a + delta * (count_b / total)
    dev = dev_a + dev_b + delta * delta * (count_a * count_b / total)
    return (total, row_average, dev)


def alternate(mlp_part, lcb_part, groups):
    rows = mlp_part.shape[0]
    return jnp.concatenate(
        [mlp_part.reshape(rows, groups, -1), lcb_part.reshape(rows, groups, -1)], axis=2
    ).reshape(rows, -1)


def on_device(embeddings, projection, compress, w_up, w_down, output_norm_gain, out_grad):
    samples = embeddings.shape[0]
    pairs = jnp.einsum(
        "sef,fk->sek", embeddings, projection, preferred_element_type=jnp.float32
    ).astype(jnp.bfloat16)
    inter = jnp.einsum(
        "sek,sef->skf", pairs, embeddings, preferred_element_type=jnp.float32
    ).reshape(samples, -1)
    center = inter - jnp.mean(inter, axis=1, keepdims=True)
    spread = jnp.mean(center * center, axis=1, keepdims=True)
    normed = (center / jnp.sqrt(spread + 1e-05)).astype(jnp.bfloat16)
    lcb = jnp.einsum(
        "sef,fj->sje", embeddings, compress, preferred_element_type=jnp.float32
    ).reshape(samples, -1)
    hidden = jax.nn.gelu(
        jnp.dot(
            lax.all_gather(normed, "tp", axis=0, tiled=True),
            w_up,
            preferred_element_type=jnp.float32,
        ),
        approximate=True,
    ).astype(jnp.bfloat16)
    group_rows = hidden.shape[0]
    tp_count = lax.axis_size("tp")
    position = lax.axis_index("tp")
    mlp = jnp.dot(hidden, w_down, preferred_element_type=jnp.float32)
    mlp_width = mlp.shape[1]
    full_width = mlp_width + lcb.shape[1]
    width = full_width // tp_count
    placed = lax.dynamic_update_slice(
        jnp.zeros((group_rows, lcb.shape[1]), jnp.float32), lcb, (position * samples, jnp.int32(0))
    )
    term = alternate(mlp, placed, tp_count)
    mixed_rows = lax.psum_scatter(
        term.astype(jnp.bfloat16), "tp", scatter_dimension=1, tiled=True
    ).astype(jnp.float32)
    own_mean = jnp.mean(mixed_rows, axis=1)
    own_dev = jnp.sum((mixed_rows - own_mean[:, None]) ** 2, axis=1)
    own_count = jnp.full((), width, jnp.float32)
    total, row_average, dev = merged((own_count, own_mean, own_dev), "tp", chan_merge)
    inverse_deviation = 1.0 / jnp.sqrt(dev[:, None] / total + 1e-05)
    centered_rows = (mixed_rows - row_average[:, None]) * inverse_deviation
    block_result = (centered_rows * output_norm_gain).astype(jnp.bfloat16)
    scaled_rows = out_grad.astype(jnp.float32) * output_norm_gain
    sum_one, sum_two = lax.psum(
        (jnp.sum(scaled_rows, axis=1), jnp.sum(scaled_rows * centered_rows, axis=1)), "tp"
    )
    first_moment = (sum_one / full_width)[:, None]
    second_moment = (sum_two / full_width)[:, None]
    local_grad = (
        (scaled_rows - first_moment - centered_rows * second_moment) * inverse_deviation
    ).astype(jnp.bfloat16)
    mixed_gradient = lax.all_gather(local_grad, "tp", axis=1, tiled=True)
    group_mlp = mlp_width // tp_count
    mlp_grad = mixed_gradient.reshape(group_rows, tp_count, -1)[:, :, :group_mlp].reshape(
        group_rows, -1
    )
    grad_down = lax.psum_scatter(
        jnp.einsum("rh,rc->hc", hidden, mlp_grad, preferred_element_type=jnp.float32).astype(
            jnp.bfloat16
        ),
        "dp",
        scatter_dimension=0,
        tiled=True,
    ).astype(jnp.float32)
    return (block_result, grad_down)


def solution(mesh):
    dp, tp = mesh.shape["dp"], mesh.shape["tp"]

    def whole(*args):
        body = functools.partial(fused_device, dp, tp) if fits(dp, tp, args) else on_device
        return jax.shard_map(
            body,
            mesh=mesh,
            in_specs=(
                P(("dp", "tp"), None, None),
                P(),
                P(),
                P(None, "tp"),
                P("tp", None),
                P("tp"),
                P("dp", "tp"),
            ),
            out_specs=(P("dp", "tp"), P(("tp", "dp"), None)),
            check_vma=False,
        )(*args)

    return whole
```
